512 devices in a mesh: dp: 16 (over z, core), fsdp: 32 (over x, y).
Axes of the slice: x: 4, y: 8, z: 8, core: 2. Of those that a mesh axis runs over, the one named last changes fastest.
Arguments:
- passages: bfloat16 [16, 32, 40, 8, 2048], P('dp', 'fsdp'), may hold values from -6 to 6
- counts: int32 [16, 32], P('dp', 'fsdp'), may hold values from 1 to 40, as said below
- helper_table: int32 [16, 32, 2, 32], P('dp', 'fsdp'), may hold values from -1 to 31, as said below
- norm_gain: float32 [2048], replicated, may hold values from 0.1 to 1.9
- projection: bfloat16 [2048, 2048], P('fsdp'), may hold values from -0.125 to 0.125
- queries: bfloat16 [16, 32, 16, 1024], P('dp', 'fsdp'), may hold values from -140 to 140
- cotangent: bfloat16 [16, 32, 24, 8, 2048], P('dp', 'fsdp'), may hold values from -0.0234375 to 0.0234375
Outputs:
- context: bfloat16 [16, 32, 16, 1024], P('dp', 'fsdp')
- gain_gradient: float32 [2048], P('fsdp')
The draws below stay inside these ranges and needn't reach their ends.
Inputs may be any that keep to these rules, and one draw needn't show every extreme that they name: `counts`: A question with passages beyond the first 8 has 8 plus that many; some question of every group has 40. `helper_table`: entries at e are -1 exactly when 8 + e is not below the question's count; otherwise row 0 names a device of the same group and row 1 a slot from 0 to 15. No two passages of a group share a device and slot; some device of every group has all 16 slots taken; one question sends at most 1 passages to one device, and some question of every group sends exactly that many to some device.
All inputs are finite; a program needn't handle non-finite values.
Results may differ from the reference program's by a relative error of at most 0.0095.
The reference program's roundings to bfloat16 on the way (of `scaled`, `states` and `weights`) count: a program that leaves them out, or rounds other values in their place, can miss the bound.
Values may be sent and summed in bfloat16 or wider, within the bound.
No kernel may reach another device: no remote copies, remote signals or barrier semaphores. Data moves between devices by JAX's collectives and lax.ppermute only.
A program may use at most 64 MiB of HBM per device.

```python
import jax
import jax.numpy as jnp
from jax import lax

D = 2048
HEADS = 32
HEAD_DIM = 32
HW = 1024
DEC = 16
LEN = 8
PMAX = 40
KEEP = 8
HELP = 16
ENC = 24
N_DP = 16
N_FSDP = 32


def plan_group(group_key):
    subkeys = jax.random.split(group_key, 5)
    spare_slots = PMAX - KEEP
    shortfall = jax.random.randint(subkeys[0], (), 0, N_FSDP)
    wanted_total = N_FSDP * HELP - shortfall
    ordering = jax.random.permutation(subkeys[1], N_FSDP)
    wishes = jax.random.randint(subkeys[2], (N_FSDP,), spare_slots // 2, spare_slots + 1)
    wishes = wishes.at[0].set(spare_slots)
    before = jnp.cumsum(wishes) - wishes
    granted = jnp.clip(wanted_total - before, 0, wishes)
    starts = jnp.cumsum(granted) - granted
    excess = jnp.zeros((N_FSDP,), jnp.int32).at[ordering].set(granted)
    start_home = jnp.zeros((N_FSDP,), jnp.int32).at[ordering].set(starts)
    baseline = jax.random.randint(subkeys[3], (N_FSDP,), 1, KEEP + 1)
    question_counts = jnp.where(excess > 0, KEEP + excess, baseline)
    helper_order = jax.random.permutation(subkeys[4], N_FSDP)
    position = jnp.arange(spare_slots, dtype=jnp.int32)
    rank_grid = start_home[:, None] + position[None, :]
    alive_grid = position[None, :] < excess[:, None]
    helpers = jnp.where(alive_grid, helper_order[rank_grid % N_FSDP], -1)
    slot_grid = jnp.where(alive_grid, rank_grid // N_FSDP, -1)
    return (question_counts.astype(jnp.int32), jnp.stack([helpers, slot_grid], axis=1).astype(jnp.int32))


def plan_slice(base_key):
    group_keys = jax.random.split(jax.random.fold_in(base_key, 29), N_DP)
    return jax.vmap(plan_group)(group_keys)


def draw_counts(key, part):
    return plan_slice(key)[0]


def draw_helper_table(key, part):
    return plan_slice(key)[1]


def draw_queries(key, part):
    subkeys = jax.random.split(jax.random.fold_in(key, 41), 1)
    full_shape = (N_DP, N_FSDP, DEC, HEADS * HEAD_DIM)
    return jax.random.normal(subkeys[0], full_shape, jnp.float32).astype(jnp.bfloat16)


def shard_levels(own_key, dims, cuts, smallest, high):
    def one(axis_at, blocks):
        steps = jax.random.uniform(jax.random.fold_in(jax.random.fold_in(own_key, 6), axis_at), (blocks,), jnp.float32, smallest / len(cuts), high / len(cuts))
        return jnp.repeat(jnp.exp(steps), dims[axis_at] // blocks).reshape((-1,) + (1,) * (len(dims) - axis_at - 1))

    level = one(*cuts[0])
    for cut in cuts[1:]:
        level = level * one(*cut)
    return level


def centred(key, dims, spread, limit, cuts=(), kind=jnp.bfloat16):
    drawn = spread * jax.random.normal(key, dims, jnp.float32)
    if cuts:
        drawn = drawn * shard_levels(key, dims, cuts, -0.22, 0.18)
    return jnp.clip(drawn, -limit, limit).astype(kind)


def setup_inputs(seed: int = 0) -> dict:
    seeds = jax.random.split(jax.random.key(seed), 8)
    return {
        "passages": centred(seeds[0], (N_DP, N_FSDP, PMAX, LEN, D), 1.0, 6.0, ((0, 16), (1, 32))),
        "counts": draw_counts(jax.random.fold_in(seeds[7], 71), 0),
        "helper_table": draw_helper_table(jax.random.fold_in(seeds[7], 71), 0),
        "norm_gain": jnp.clip(1.0 + 0.18 * jax.random.normal(seeds[3], (D,), jnp.float32), 0.1, 1.9),
        "projection": centred(seeds[4], (D, 2 * HW), D ** -0.5, 0.125, ((0, 32),)),
        "queries": draw_queries(jax.random.fold_in(seeds[7], 71), 0),
        "cotangent": centred(seeds[6], (N_DP, N_FSDP, ENC, LEN, 2 * HW), 0.004, 0.0234375, ((0, 16), (1, 32))),
    }


EPSILON = 1e-06

def normalize(states):
    values = states.astype(jnp.float32)
    scaling = lax.rsqrt(lax.optimization_barrier(jnp.mean(values * values, axis=-1, keepdims=True)) + EPSILON)
    return values * scaling

def attend(query_rows, state_rows, token_live):
    key_rows = state_rows[:, :HW].reshape(-1, HEADS, HEAD_DIM).astype(jnp.float32)
    value_rows = state_rows[:, HW:].reshape(-1, HEADS, HEAD_DIM).astype(jnp.float32)
    query_values = query_rows.reshape(DEC, HEADS, HEAD_DIM).astype(jnp.float32)
    scores = jnp.einsum('qhd,thd->hqt', query_values, key_rows) * HEAD_DIM ** (-0.5)
    scores = jnp.where(token_live[None, None, :], scores, -jnp.inf)
    highest = lax.optimization_barrier(jnp.max(scores, axis=-1, keepdims=True))
    raised = jnp.exp(scores - highest)
    weights = (raised / lax.optimization_barrier(jnp.sum(raised, axis=-1, keepdims=True))).astype(jnp.bfloat16)
    context = jnp.einsum('hqt,thd->qhd', weights.astype(jnp.float32), value_rows)
    return context.reshape(DEC, HW).astype(jnp.bfloat16)

def reference(passages, counts, helper_table, norm_gain, projection, queries, cotangent):
    devices_total = N_DP * N_FSDP
    device_ids = jnp.arange(devices_total, dtype=jnp.int32)
    group_start = device_ids // N_FSDP * N_FSDP
    table_rows = helper_table.reshape(devices_total, 2, PMAX - KEEP).astype(jnp.int32)
    local_index = device_ids[:, None] * ENC + jnp.arange(KEEP, dtype=jnp.int32)[None, :]
    remote_index = (group_start[:, None] + jnp.maximum(table_rows[:, 0], 0)) * ENC + KEEP + jnp.maximum(table_rows[:, 1], 0)
    source_index = jnp.concatenate([local_index, remote_index], axis=1).astype(jnp.int32)
    upstream_all = cotangent.reshape(devices_total * ENC, LEN * 2 * HW)
    passage_ids = jnp.arange(PMAX, dtype=jnp.int32)

    def one_question(inputs):
        stored, passage_count, source_rows, query_rows = inputs
        normal = normalize(stored).reshape(PMAX * LEN, D)
        scaled = (normal * norm_gain.astype(jnp.float32)).astype(jnp.bfloat16)
        states = jnp.dot(scaled, projection, preferred_element_type=jnp.float32).astype(jnp.bfloat16)
        token_live = jnp.repeat(passage_ids < passage_count, LEN)
        context = attend(query_rows, states, token_live)
        upstream = jnp.take(upstream_all, source_rows, axis=0).reshape(PMAX * LEN, 2 * HW)
        back_rows = jnp.dot(upstream, projection.T, preferred_element_type=jnp.float32)
        mask_column = token_live.astype(jnp.float32)[:, None]
        row_terms = lax.optimization_barrier(jnp.sum(normal * back_rows * mask_column, axis=0))
        return (context, row_terms)
    contexts, terms_all = lax.map(one_question, (passages.reshape(devices_total, PMAX, LEN, D), counts.reshape(devices_total), source_index, queries.reshape(devices_total, DEC, HW)))
    return (contexts.reshape(N_DP, N_FSDP, DEC, HW), lax.optimization_barrier(jnp.sum(terms_all, axis=0)))
```

```python
import jax
import jax.numpy as jnp
from jax import lax
from jax.experimental import pallas as pl
from jax.experimental.pallas import tpu as pltpu
from jax.sharding import Mesh
from jax.sharding import PartitionSpec as P

D = 2048
HEADS = 32
HEAD_DIM = 32
HW = 1024
DEC = 16
LEN = 8
PMAX = 40
KEEP = 8
HELP = 16
ENC = 24
TOK = PMAX * LEN
OWN = KEEP * LEN
AID = HELP * LEN
G = 4
COLS = HW // G
GH = HEADS // G
QROW = ENC * LEN
CROW = QROW + DEC
EROWS = CROW + 16
WIDE = D + 128
EPSILON = 1e-06
GROUP = ("zl", "core")
DP = ("zh", "zl", "core")
FSDP = ("x", "y")

VM = pl.BlockSpec(memory_space=pltpu.VMEM)
SM = pl.BlockSpec(memory_space=pltpu.SMEM)


def params():
    return pltpu.CompilerParams(vmem_limit_bytes=48 * 1024 * 1024)


def pack_body(table, passages, out):
    for s in range(32):
        out[s, :, D:] = jnp.full((LEN, WIDE - D), -1.0, jnp.bfloat16)
    for e in range(PMAX - KEEP):
        peer = table[0, e]

        @pl.when(peer >= 0)
        def _():
            slot = table[1, e].astype(jnp.float32)
            out[peer, :, :D] = passages[KEEP + e]
            out[peer, :, D:] = jnp.full((LEN, WIDE - D), slot, jnp.float32).astype(jnp.bfloat16)


def pack(table, passages):
    return pl.pallas_call(
        pack_body,
        out_shape=jax.ShapeDtypeStruct((32, LEN, WIDE), jnp.bfloat16),
        in_specs=[SM, VM],
        out_specs=VM,
        compiler_params=params(),
        name="pack",
    )(table, passages)


def prep_body(count, cot, queries, out):
    for g in range(G):
        lo, hi = g * COLS, (g + 1) * COLS
        out[g, :QROW, :COLS] = cot[:, lo:hi]
        out[g, :QROW, COLS:] = cot[:, HW + lo : HW + hi]
        out[g, QROW:CROW, :COLS] = queries[:, lo:hi]
        out[g, QROW:CROW, COLS:] = queries[:, lo:hi]
        out[g, CROW:, :] = jnp.full((EROWS - CROW, 2 * COLS), count[0].astype(jnp.float32), jnp.float32).astype(
            jnp.bfloat16
        )


def prep(count, cot, queries):
    return pl.pallas_call(
        prep_body,
        out_shape=jax.ShapeDtypeStruct((G, EROWS, 2 * COLS), jnp.bfloat16),
        in_specs=[SM, VM, VM],
        out_specs=VM,
        compiler_params=params(),
        name="prep",
    )(count, cot, queries)


def unpack_body(tags, arrived, out):
    out[...] = jnp.zeros(out.shape, out.dtype)
    for s in range(32):
        tag = tags[s]

        @pl.when(tag >= 0)
        def _():
            out[tag] = arrived[s, :, :D]


def unpack(tags, arrived):
    return pl.pallas_call(
        unpack_body,
        out_shape=jax.ShapeDtypeStruct((HELP, LEN, D), jnp.bfloat16),
        in_specs=[SM, VM],
        out_specs=VM,
        compiler_params=params(),
        name="unpack",
    )(tags, arrived)


def normal_of(values):
    return values * lax.rsqrt(jnp.mean(values * values, axis=-1, keepdims=True) + EPSILON)


def normals_body(member, e, x0, x1, x2, x3, h0, h1, h2, h3, out):
    for r, (x, h) in enumerate(((x0, h0), (x1, h1), (x2, h2), (x3, h3))):
        src = member[0] ^ r
        live = e[src, CROW : CROW + 8, :128].astype(jnp.float32)[0:1, 0:1]
        spot = (lax.broadcasted_iota(jnp.int32, (OWN, 1), 0) // LEN).astype(jnp.float32)
        normal = normal_of(x[...].astype(jnp.float32))
        out[src, :OWN, :] = jnp.where(spot < live, normal, 0.0)
        out[src, OWN:, :] = normal_of(h[...].astype(jnp.float32))


def normals(member, e, xs, hs):
    return pl.pallas_call(
        normals_body,
        out_shape=jax.ShapeDtypeStruct((G, QROW, D), jnp.float32),
        grid=(1,),
        in_specs=[SM, pl.BlockSpec((G, EROWS, 2 * COLS), lambda i: (0, 0, 0))]
        + [pl.BlockSpec((OWN, D), lambda i: (0, 0))] * G
        + [pl.BlockSpec((AID, D), lambda i: (0, 0))] * G,
        out_specs=pl.BlockSpec((G, QROW, D), lambda i: (0, 0, 0)),
        compiler_params=params(),
        name="normals",
    )(member, e, *xs, *hs)


def grad_body(e, normal, weight, out):
    cot = e[:, :QROW, :].reshape(G * QROW, 2 * COLS)
    back = lax.dot_general(cot, weight[...], (((1,), (1,)), ((), ())), preferred_element_type=jnp.float32)
    block = normal.shape[-1]
    out[...] = jnp.sum(normal[...].reshape(G * QROW, block) * back, axis=0, keepdims=True)


def grad(e, normal, weight):
    block = 512
    return pl.pallas_call(
        grad_body,
        out_shape=jax.ShapeDtypeStruct((1, D), jnp.float32),
        grid=(D // block,),
        in_specs=[
            pl.BlockSpec((G, EROWS, 2 * COLS), lambda i: (0, 0, 0)),
            pl.BlockSpec((G, QROW, block), lambda i: (0, 0, i)),
            pl.BlockSpec((block, 2 * COLS), lambda i: (i, 0)),
        ],
        out_specs=pl.BlockSpec((1, block), lambda i: (0, i)),
        compiler_params=params(),
        name="gain_grad",
    )(e, normal, weight)


def attend_body(member, e, gain, weight, x0, x1, x2, x3, out):
    rows = GH * DEC
    row_head = lax.broadcasted_iota(jnp.int32, (rows, COLS), 0) // DEC
    col_head = lax.broadcasted_iota(jnp.int32, (rows, COLS), 1) // HEAD_DIM
    same = row_head == col_head
    spot = (lax.broadcasted_iota(jnp.int32, (1, TOK), 1) // LEN).astype(jnp.float32)
    for r, x in enumerate((x0, x1, x2, x3)):
        src = member[0] ^ r
        scaled = (normal_of(x[...].astype(jnp.float32)) * gain[...]).astype(jnp.bfloat16)
        states = jnp.dot(scaled, weight[...], preferred_element_type=jnp.float32).astype(jnp.bfloat16)
        query = e[src, QROW:CROW, :COLS].astype(jnp.float32)
        spread = jnp.where(same, jnp.concatenate([query] * GH, axis=0), 0.0).astype(jnp.bfloat16)
        scores = lax.dot_general(
            spread, states[:, :COLS], (((1,), (1,)), ((), ())), preferred_element_type=jnp.float32
        ) * HEAD_DIM ** (-0.5)
        count = e[src, CROW : CROW + 8, :TOK].astype(jnp.float32)[0:1, :]
        scores = jnp.where(spot < count, scores, -jnp.inf)
        raised = jnp.exp(scores - jnp.max(scores, axis=-1, keepdims=True))
        weights = (raised / jnp.sum(raised, axis=-1, keepdims=True)).astype(jnp.bfloat16)
        mixed = jnp.dot(weights, states[:, COLS:], preferred_element_type=jnp.float32)
        mixed = jnp.where(same, mixed, 0.0).reshape(GH, DEC, COLS)
        out[src] = jnp.sum(mixed, axis=0).astype(jnp.bfloat16)


def attend(member, e, gain, weight, xs):
    return pl.pallas_call(
        attend_body,
        out_shape=jax.ShapeDtypeStruct((G, DEC, COLS), jnp.bfloat16),
        in_specs=[SM, VM, VM, VM, VM, VM, VM, VM],
        out_specs=VM,
        compiler_params=params(),
        name="attend",
    )(member, e, gain, weight, *xs)


def exchange(array, axes):
    return lax.all_to_all(array, axes, 0, 0, tiled=True)


def spread_to(array, axis):
    return exchange(jnp.broadcast_to(array[None], (lax.axis_size(axis), *array.shape)), axis)


def swap(array, axis):
    return lax.ppermute(array, axis, [(0, 1), (1, 0)])


def shards(passages, counts, helper_table, norm_gain, projection, queries, cotangent):
    member = (lax.axis_index("zl") * 2 + lax.axis_index("core")).astype(jnp.int32)
    stored = passages.reshape(PMAX, LEN, D)
    x_own = passages.reshape(TOK, D)
    member_ref = member.reshape(1)

    x_z = swap(x_own, "zl")
    x_c = swap(x_own, "core")
    x_cz = swap(x_z, "core")
    xs = (x_own, x_c, x_z, x_cz)

    outgoing = pack(helper_table.reshape(2, PMAX - KEEP), stored)
    arrived = exchange(outgoing, FSDP)
    e = exchange(prep(counts.reshape(1), cotangent.reshape(QROW, D), queries.reshape(DEC, HW)), GROUP)

    tags = arrived[:, 0, D].astype(jnp.int32)
    h_own = unpack(tags, arrived).reshape(AID, D)
    h_z = swap(h_own, "zl")
    h_c = swap(h_own, "core")
    h_cz = swap(h_z, "core")
    normal = normals(member_ref, e, xs, (h_own, h_c, h_z, h_cz))

    mine = lax.dynamic_index_in_dim(projection.reshape(64, 2, G, COLS), member, 2, keepdims=False).reshape(
        64, 2 * COLS
    )
    by_y = spread_to(mine, "y").reshape(512, 2 * COLS)
    weight = spread_to(by_y, "x").reshape(D, 2 * COLS)

    row_terms = grad(e, normal, weight)
    parts = exchange(row_terms.reshape(32, 1, 64), FSDP)
    share = jnp.sum(parts, axis=0)
    gathered = exchange(jnp.broadcast_to(share[None], (16, 1, 64)), DP)
    gradient = jnp.sum(gathered, axis=0).reshape(64)

    mixed = attend(member_ref, e, norm_gain.reshape(1, D), weight, xs)
    context = exchange(mixed, GROUP)
    context_out = jnp.transpose(context, (1, 0, 2)).reshape(1, 1, DEC, HW)
    return (context_out, gradient)


def solution(mesh):
    split = Mesh(mesh.devices.reshape(4, 2, 2, 4, 8), ("zh", "zl", "core", "x", "y"))
    return jax.shard_map(
        shards,
        mesh=split,
        in_specs=(
            P(DP, FSDP, None, None, None),
            P(DP, FSDP),
            P(DP, FSDP, None, None),
            P(),
            P(FSDP, None),
            P(DP, FSDP, None, None),
            P(DP, FSDP, None, None, None),
        ),
        out_specs=(P(DP, FSDP, None, None), P(FSDP)),
        check_vma=False,
    )
```

```python
import jax
import jax.numpy as jnp
from jax import lax
from jax.experimental import pallas as pl
from jax.experimental.pallas import tpu as pltpu
from jax.sharding import Mesh
from jax.sharding import PartitionSpec as P

D = 2048
HEADS = 32
HEAD_DIM = 32
HW = 1024
DEC = 16
LEN = 8
PMAX = 40
KEEP = 8
HELP = 16
ENC = 24
TOK = PMAX * LEN
OWN = KEEP * LEN
AID = HELP * LEN
G = 4
COLS = HW // G
GH = HEADS // G
CROW = TOK + ENC * LEN // 2
QROW = CROW
MROWS = QROW + DEC
WIDE = D + 128
EPSILON = 1e-06
GROUP = ("zl", "core")
DP = ("zh", "zl", "core")
FSDP = ("x", "y")

VM = pl.BlockSpec(memory_space=pltpu.VMEM)
SM = pl.BlockSpec(memory_space=pltpu.SMEM)


def params():
    return pltpu.CompilerParams(vmem_limit_bytes=48 * 1024 * 1024)


def pack_body(table, passages, out):
    for s in range(32):
        out[s, :, D:] = jnp.full((LEN, WIDE - D), -1.0, jnp.bfloat16)
    for e in range(PMAX - KEEP):
        peer = table[0, e]

        @pl.when(peer >= 0)
        def _():
            slot = table[1, e].astype(jnp.float32)
            out[peer, :, :D] = passages[KEEP + e]
            out[peer, :, D:] = jnp.full((LEN, WIDE - D), slot, jnp.float32).astype(jnp.bfloat16)


def pack(table, passages):
    return pl.pallas_call(
        pack_body,
        out_shape=jax.ShapeDtypeStruct((32, LEN, WIDE), jnp.bfloat16),
        in_specs=[SM, VM],
        out_specs=VM,
        compiler_params=params(),
        name="pack",
    )(table, passages)


def prep_body(place, count, passages, cot, queries, near, far):
    half = ENC * LEN // 2
    for out, flip in ((near, 0), (far, 1)):
        out[:TOK, :] = passages[...]
        for z in range(2):

            @pl.when(place[0] == z)
            def _():
                for c in range(2):
                    lo = (2 * (z ^ flip) + c) * COLS
                    for part in range(2):
                        at = (2 * c + part) * 2 * COLS
                        rows = slice(part * half, (part + 1) * half)
                        out[TOK:CROW, at : at + COLS] = cot[rows, lo : lo + COLS]
                        out[TOK:CROW, at + COLS : at + 2 * COLS] = cot[rows, HW + lo : HW + lo + COLS]
                    out[QROW:, c * COLS : (c + 1) * COLS] = queries[:, lo : lo + COLS]

        out[QROW:, 2 * COLS :] = jnp.full((DEC, D - 2 * COLS), count[0].astype(jnp.float32), jnp.float32).astype(
            jnp.bfloat16
        )


def prep(place, count, passages, cot, queries):
    message = jax.ShapeDtypeStruct((MROWS, D), jnp.bfloat16)
    return pl.pallas_call(
        prep_body,
        out_shape=(message, message),
        in_specs=[SM, SM, VM, VM, VM],
        out_specs=(VM, VM),
        compiler_params=params(),
        name="prep",
    )(place, count, passages, cot, queries)


def columns_body(member, projection, out):
    for g in range(G):

        @pl.when(member[0] == g)
        def _():
            lo = g * COLS
            for peer in range(8):
                out[peer, :, :COLS] = projection[:, lo : lo + COLS]
                out[peer, :, COLS:] = projection[:, HW + lo : HW + lo + COLS]


def columns(member, projection):
    return pl.pallas_call(
        columns_body,
        out_shape=jax.ShapeDtypeStruct((8, 64, 2 * COLS), jnp.bfloat16),
        in_specs=[SM, VM],
        out_specs=VM,
        compiler_params=params(),
        name="columns",
    )(member, projection)


def unpack_body(tags, arrived, out):
    out[...] = jnp.zeros(out.shape, out.dtype)
    for s in range(32):
        tag = tags[s]

        @pl.when(tag >= 0)
        def _():
            out[tag] = arrived[s, :, :D]


def unpack(tags, arrived):
    return pl.pallas_call(
        unpack_body,
        out_shape=jax.ShapeDtypeStruct((HELP, LEN, D), jnp.bfloat16),
        in_specs=[SM, VM],
        out_specs=VM,
        compiler_params=params(),
        name="unpack",
    )(tags, arrived)


def inverse_rms(values):
    return lax.rsqrt(jnp.mean(values * values, axis=-1, keepdims=True) + EPSILON)


def scale_body(message, gain, out):
    values = message[...].astype(jnp.float32)
    out[...] = (values * inverse_rms(values) * gain[...]).astype(jnp.bfloat16)


def scale(message, gain):
    return pl.pallas_call(
        scale_body,
        out_shape=jax.ShapeDtypeStruct((TOK, D), jnp.bfloat16),
        grid=(1,),
        in_specs=[pl.BlockSpec((TOK, D), lambda i: (0, 0)), pl.BlockSpec((1, D), lambda i: (0, 0))],
        out_specs=pl.BlockSpec((TOK, D), lambda i: (0, 0)),
        compiler_params=params(),
        name="scale",
    )(message, gain)


def outer_body(place, m0, m1, m2, m3, h0, h1, h2, h3, out, rows, high, low):
    spot = (lax.broadcasted_iota(jnp.int32, (OWN, 1), 0) // LEN).astype(jnp.float32)
    for r, (message, aid) in enumerate(((m0, h0), (m1, h1), (m2, h2), (m3, h3))):
        at = r * ENC * LEN
        own = message[:OWN, :]
        helped = aid[...]
        rows[at : at + OWN, :] = own
        rows[at + OWN : at + ENC * LEN, :] = helped
        count = message[QROW : QROW + DEC, 2 * COLS : 2 * COLS + 128].astype(jnp.float32)[0:1, 0:1]
        own_scale = jnp.where(spot < count, inverse_rms(own.astype(jnp.float32)), 0.0)
        scales = jnp.concatenate([own_scale, inverse_rms(helped.astype(jnp.float32))], axis=0)
        for c in range(2):

            @pl.when(place[1] == c)
            def _():
                left = 4 * c * COLS
                cot = jnp.concatenate(
                    [
                        message[TOK:CROW, left : left + 2 * COLS],
                        message[TOK:CROW, left + 2 * COLS : left + 4 * COLS],
                    ],
                    axis=0,
                )
                product = cot.astype(jnp.float32) * scales
                top = product.astype(jnp.bfloat16)
                high[at : at + ENC * LEN, :] = top
                low[at : at + ENC * LEN, :] = (product - top.astype(jnp.float32)).astype(jnp.bfloat16)

    over_tokens = (((0,), (0,)), ((), ()))
    block = 512
    for d in range(0, D, block):
        x = rows[:, d : d + block]
        out[d : d + block, :] = lax.dot_general(
            x, high[...], over_tokens, preferred_element_type=jnp.float32
        ) + lax.dot_general(x, low[...], over_tokens, preferred_element_type=jnp.float32)


def outer(place, messages, hs):
    return pl.pallas_call(
        outer_body,
        out_shape=jax.ShapeDtypeStruct((D, 2 * COLS), jnp.float32),
        in_specs=[SM] + [VM] * (2 * G),
        out_specs=VM,
        scratch_shapes=[
            pltpu.VMEM((G * ENC * LEN, D), jnp.bfloat16),
            pltpu.VMEM((G * ENC * LEN, 2 * COLS), jnp.bfloat16),
            pltpu.VMEM((G * ENC * LEN, 2 * COLS), jnp.bfloat16),
        ],
        compiler_params=params(),
        name="outer",
    )(place, *messages, *hs)


def grad_body(weight, products, out):
    out[...] = jnp.sum((weight[...].astype(jnp.float32) * products[...]).reshape(32, 64, 2 * COLS), axis=-1)


def grad(weight, products):
    return pl.pallas_call(
        grad_body,
        out_shape=jax.ShapeDtypeStruct((32, 64), jnp.float32),
        in_specs=[VM, VM],
        out_specs=VM,
        compiler_params=params(),
        name="gain_grad",
    )(weight, products)


def attend_body(place, weight, m0, m1, m2, m3, s0, s1, s2, s3, out):
    rows = GH * DEC
    row_head = lax.broadcasted_iota(jnp.int32, (rows, COLS), 0) // DEC
    col_head = lax.broadcasted_iota(jnp.int32, (rows, COLS), 1) // HEAD_DIM
    same = row_head == col_head
    spot = (lax.broadcasted_iota(jnp.int32, (1, TOK), 1) // LEN).astype(jnp.float32)
    upper = place[1] == 1
    for r, (message, scaled) in enumerate(((m0, s0), (m1, s1), (m2, s2), (m3, s3))):
        states = jnp.dot(scaled[...], weight[...], preferred_element_type=jnp.float32).astype(jnp.bfloat16)
        query = jnp.where(
            upper,
            message[:, COLS : 2 * COLS].astype(jnp.float32),
            message[:, :COLS].astype(jnp.float32),
        )
        spread = jnp.where(same, jnp.concatenate([query] * GH, axis=0), 0.0).astype(jnp.bfloat16)
        scores = lax.dot_general(
            spread, states[:, :COLS], (((1,), (1,)), ((), ())), preferred_element_type=jnp.float32
        ) * HEAD_DIM ** (-0.5)
        count = message[:, 2 * COLS : 2 * COLS + TOK].astype(jnp.float32)[0:1, :]
        scores = jnp.where(spot < count, scores, -jnp.inf)
        raised = jnp.exp(scores - jnp.max(scores, axis=-1, keepdims=True))
        weights = (raised / jnp.sum(raised, axis=-1, keepdims=True)).astype(jnp.bfloat16)
        mixed = jnp.dot(weights, states[:, COLS:], preferred_element_type=jnp.float32)
        mixed = jnp.where(same, mixed, 0.0).reshape(GH, DEC, COLS)
        out[(2 * place[0] + place[1]) ^ r] = jnp.sum(mixed, axis=0).astype(jnp.bfloat16)


def attend(place, weight, messages, scaled):
    last = pl.BlockSpec((DEC, D), lambda i: (QROW // DEC, 0))
    return pl.pallas_call(
        attend_body,
        out_shape=jax.ShapeDtypeStruct((G, DEC, COLS), jnp.bfloat16),
        grid=(1,),
        in_specs=[SM, pl.BlockSpec((D, 2 * COLS), lambda i: (0, 0))]
        + [last] * G
        + [pl.BlockSpec((TOK, D), lambda i: (0, 0))] * G,
        out_specs=pl.BlockSpec((G, DEC, COLS), lambda i: (0, 0, 0)),
        compiler_params=params(),
        name="attend",
    )(place, weight, *messages, *scaled)


def exchange(array, axes):
    return lax.all_to_all(array, axes, 0, 0, tiled=True)


def spread_to(array, axis):
    return exchange(jnp.broadcast_to(array[None], (lax.axis_size(axis), *array.shape)), axis)


def swap(array, axis):
    return lax.ppermute(array, axis, [(0, 1), (1, 0)])


def forward(passages, counts, helper_table, norm_gain, projection, queries, cotangent):
    zl, core = lax.axis_index("zl").astype(jnp.int32), lax.axis_index("core").astype(jnp.int32)
    place = jnp.stack([zl, core])
    member = (zl * 2 + core).reshape(1)
    gain = norm_gain.reshape(1, D)

    near, far = prep(
        place, counts.reshape(1), passages.reshape(TOK, D), cotangent.reshape(ENC * LEN, D), queries.reshape(DEC, HW)
    )
    m_z = swap(far, "zl")
    m_c = swap(near, "core")
    m_cz = swap(m_z, "core")
    messages = (near, m_c, m_z, m_cz)

    outgoing = pack(helper_table.reshape(2, PMAX - KEEP), passages.reshape(PMAX, LEN, D))
    arrived = exchange(outgoing, FSDP)
    s_0, s_1 = scale(near, gain), scale(m_c, gain)
    tags = arrived[:, 0, D].astype(jnp.int32)
    h_own = unpack(tags, arrived).reshape(AID, D)
    h_z = swap(h_own, "zl")
    h_c = swap(h_own, "core")
    h_cz = swap(h_z, "core")

    mine = columns(member, projection)
    mine, s_0, s_1, _ = lax.optimization_barrier((mine, s_0, s_1, h_own))
    by_y = exchange(mine, "y").reshape(512, 2 * COLS)
    weight = spread_to(by_y, "x").reshape(D, 2 * COLS)
    s_2, s_3 = scale(m_z, gain), scale(m_cz, gain)
    products = outer(place, messages, (h_own, h_c, h_z, h_cz))
    weight, s_2, s_3, products = lax.optimization_barrier((weight, s_2, s_3, products))
    scaled = (s_0, s_1, s_2, s_3)

    row_terms = grad(weight, products)
    parts = exchange(row_terms.reshape(32, 1, 64), FSDP)
    share = jnp.sum(parts, axis=0)
    gathered = exchange(jnp.broadcast_to(share[None], (16, 1, 64)), DP)
    gradient = jnp.sum(gathered, axis=0).reshape(64)

    context = exchange(attend(place, weight, messages, scaled), GROUP)
    context_out = jnp.transpose(context, (1, 0, 2)).reshape(1, 1, DEC, HW)
    return (context_out, gradient)


def solution(mesh):
    split = Mesh(mesh.devices.reshape(4, 2, 2, 4, 8), ("zh", "zl", "core", "x", "y"))
    return jax.shard_map(
        forward,
        mesh=split,
        in_specs=(
            P(DP, FSDP, None, None, None),
            P(DP, FSDP),
            P(DP, FSDP, None, None),
            P(),
            P(FSDP, None),
            P(DP, FSDP, None, None),
            P(DP, FSDP, None, None, None),
        ),
        out_specs=(P(DP, FSDP, None, None), P(FSDP)),
        check_vma=False,
    )
```

```python
import jax
import jax.numpy as jnp
from jax import lax
from jax.experimental import pallas as pl
from jax.experimental.pallas import tpu as pltpu
from jax.sharding import Mesh
from jax.sharding import PartitionSpec as P

D = 2048
HEADS = 32
HEAD_DIM = 32
HW = 1024
DEC = 16
LEN = 8
PMAX = 40
KEEP = 8
HELP = 16
ENC = 24
TOK = PMAX * LEN
OWN = KEEP * LEN
AID = HELP * LEN
G = 4
COLS = HW // G
GH = HEADS // G
CROW = TOK + ENC * LEN // 2
QROW = CROW
MROWS = QROW + DEC
WIDE = D + 128
EPSILON = 1e-06
CHUNKS = 4
GROUP = ("zl", "core")
DP = ("zh", "zl", "core")
FSDP = ("x", "y")

VM = pl.BlockSpec(memory_space=pltpu.VMEM)
SM = pl.BlockSpec(memory_space=pltpu.SMEM)
HB = pl.BlockSpec(memory_space=pltpu.HBM)


def in_hbm(array):
    return pltpu.with_memory_space_constraint(array, pltpu.HBM)


def params():
    return pltpu.CompilerParams(vmem_limit_bytes=24 * 1024 * 1024)


def pack_body(table, passages, out, arrivals):
    def copy(e):
        peer = jnp.maximum(table[0, e], 0)
        return pltpu.make_async_copy(passages.at[KEEP + e], out.at[peer, :, pl.ds(0, D)], arrivals.at[e])

    for e in range(PMAX - KEEP):

        @pl.when(table[0, e] >= 0)
        def _():
            copy(e).start()

    for s in range(32):
        out[s, :, D:] = jnp.full((LEN, WIDE - D), -1.0, jnp.bfloat16)
    for e in range(PMAX - KEEP):
        peer = table[0, e]

        @pl.when(peer >= 0)
        def _():
            slot = table[1, e].astype(jnp.float32)
            out[peer, :, D:] = jnp.full((LEN, WIDE - D), slot, jnp.float32).astype(jnp.bfloat16)

    for e in range(PMAX - KEEP):

        @pl.when(table[0, e] >= 0)
        def _():
            copy(e).wait()


def pack(table, passages):
    return pl.pallas_call(
        pack_body,
        out_shape=jax.ShapeDtypeStruct((32, LEN, WIDE), jnp.bfloat16),
        in_specs=[SM, HB],
        out_specs=VM,
        scratch_shapes=[pltpu.SemaphoreType.DMA((PMAX - KEEP,))],
        compiler_params=params(),
        name="pack",
    )(table, in_hbm(passages))


def prep_body(place, count, passages, cot, queries, near, far):
    half = ENC * LEN // 2
    for out, flip in ((near, 0), (far, 1)):
        out[:TOK, :] = passages[...]
        for z in range(2):

            @pl.when(place[0] == z)
            def _():
                for c in range(2):
                    lo = (2 * (z ^ flip) + c) * COLS
                    for part in range(2):
                        at = (2 * c + part) * 2 * COLS
                        rows = slice(part * half, (part + 1) * half)
                        out[TOK:CROW, at : at + COLS] = cot[rows, lo : lo + COLS]
                        out[TOK:CROW, at + COLS : at + 2 * COLS] = cot[rows, HW + lo : HW + lo + COLS]
                    out[QROW:, c * COLS : (c + 1) * COLS] = queries[:, lo : lo + COLS]

        out[QROW:, 2 * COLS :] = jnp.full((DEC, D - 2 * COLS), count[0].astype(jnp.float32), jnp.float32).astype(
            jnp.bfloat16
        )


def prep(place, count, passages, cot, queries):
    message = jax.ShapeDtypeStruct((MROWS, D), jnp.bfloat16)
    return pl.pallas_call(
        prep_body,
        out_shape=(message, message),
        in_specs=[SM, SM, VM, VM, VM],
        out_specs=(VM, VM),
        compiler_params=params(),
        name="prep",
    )(place, count, passages, cot, queries)


def columns_body(member, projection, out):
    for g in range(G):

        @pl.when(member[0] == g)
        def _():
            lo = g * COLS
            for peer in range(8):
                out[peer, :, :COLS] = projection[:, lo : lo + COLS]
                out[peer, :, COLS:] = projection[:, HW + lo : HW + lo + COLS]


def columns(member, projection):
    return pl.pallas_call(
        columns_body,
        out_shape=jax.ShapeDtypeStruct((8, 64, 2 * COLS), jnp.bfloat16),
        in_specs=[SM, VM],
        out_specs=VM,
        compiler_params=params(),
        name="columns",
    )(member, projection)


def unpack_body(tags, arrived, out):
    out[...] = jnp.zeros(out.shape, out.dtype)
    for s in range(32):
        tag = tags[s]

        @pl.when(tag >= 0)
        def _():
            out[tag] = arrived[s, :, :D]


def unpack(tags, arrived):
    return pl.pallas_call(
        unpack_body,
        out_shape=jax.ShapeDtypeStruct((HELP, LEN, D), jnp.bfloat16),
        in_specs=[SM, VM],
        out_specs=VM,
        compiler_params=params(),
        name="unpack",
    )(tags, arrived)


def inverse_rms(values):
    return lax.rsqrt(jnp.mean(values * values, axis=-1, keepdims=True) + EPSILON)


def outer_body(place, m0, m1, m2, m3, h0, h1, h2, h3, out, rows, tails, high, low, total, arrivals, leaving):
    messages = (m0, m1, m2, m3)
    size = ENC * LEN
    copies = []
    for r, message in enumerate(messages):
        own = pltpu.make_async_copy(message.at[pl.ds(0, OWN)], rows.at[pl.ds(r * size, OWN)], arrivals.at[r, 0])
        tail = pltpu.make_async_copy(message.at[pl.ds(TOK, MROWS - TOK)], tails.at[r], arrivals.at[r, 1])
        own.start()
        tail.start()
        copies.append((own, tail))
    spot = (lax.broadcasted_iota(jnp.int32, (OWN, 1), 0) // LEN).astype(jnp.float32)
    for r, aid in enumerate((h0, h1, h2, h3)):
        at = r * size
        helped = aid[...]
        rows[at + OWN : at + size, :] = helped
        helped_scale = inverse_rms(helped.astype(jnp.float32))
        for copy in copies[r]:
            copy.wait()
        count = tails[r, QROW - TOK :, 2 * COLS : 2 * COLS + 128].astype(jnp.float32)[0:1, 0:1]
        own_scale = jnp.where(spot < count, inverse_rms(rows[at : at + OWN, :].astype(jnp.float32)), 0.0)
        scales = jnp.concatenate([own_scale, helped_scale], axis=0)
        for c in range(2):

            @pl.when(place[1] == c)
            def _():
                left = 4 * c * COLS
                cot = jnp.concatenate(
                    [
                        tails[r, : CROW - TOK, left : left + 2 * COLS],
                        tails[r, : CROW - TOK, left + 2 * COLS : left + 4 * COLS],
                    ],
                    axis=0,
                )
                product = cot.astype(jnp.float32) * scales
                top = product.astype(jnp.bfloat16)
                high[at : at + size, :] = top
                low[at : at + size, :] = (product - top.astype(jnp.float32)).astype(jnp.bfloat16)

    over_tokens = (((0,), (0,)), ((), ()))
    block = D // CHUNKS
    sent = []
    for i in range(CHUNKS):
        d = i * block
        x = rows[:, d : d + block]
        total[d : d + block, :] = lax.dot_general(
            x, high[...], over_tokens, preferred_element_type=jnp.float32
        ) + lax.dot_general(x, low[...], over_tokens, preferred_element_type=jnp.float32)
        leave = pltpu.make_async_copy(total.at[pl.ds(d, block)], out.at[pl.ds(d, block)], leaving.at[i])
        leave.start()
        sent.append(leave)
    for leave in sent:
        leave.wait()


def outer(place, messages, hs):
    return pl.pallas_call(
        outer_body,
        out_shape=pltpu.HBM((D, 2 * COLS), jnp.float32),
        in_specs=[SM] + [HB] * G + [VM] * G,
        out_specs=HB,
        scratch_shapes=[
            pltpu.VMEM((G * ENC * LEN, D), jnp.bfloat16),
            pltpu.VMEM((G, MROWS - TOK, D), jnp.bfloat16),
            pltpu.VMEM((G * ENC * LEN, 2 * COLS), jnp.bfloat16),
            pltpu.VMEM((G * ENC * LEN, 2 * COLS), jnp.bfloat16),
            pltpu.VMEM((D, 2 * COLS), jnp.float32),
            pltpu.SemaphoreType.DMA((G, 2)),
            pltpu.SemaphoreType.DMA((CHUNKS,)),
        ],
        compiler_params=params(),
        name="outer_product",
    )(place, *map(in_hbm, messages), *hs)


def grad_body(weight, products, out, held, arrivals):
    block = D // CHUNKS
    copies = []
    for i in range(CHUNKS):
        span = pl.ds(i * block, block)
        copy = pltpu.make_async_copy(products.at[span], held.at[span], arrivals.at[i])
        copy.start()
        copies.append(copy)
    for i in range(CHUNKS):
        copies[i].wait()
        at = slice(i * block, (i + 1) * block)
        terms = weight[at, :].astype(jnp.float32) * held[at, :]
        out[i * block // 64 : (i + 1) * block // 64, :] = jnp.sum(terms.reshape(block // 64, 64, 2 * COLS), axis=-1)


def grad(weight, products):
    return pl.pallas_call(
        grad_body,
        out_shape=jax.ShapeDtypeStruct((32, 64), jnp.float32),
        in_specs=[VM, HB],
        out_specs=VM,
        scratch_shapes=[pltpu.VMEM((D, 2 * COLS), jnp.float32), pltpu.SemaphoreType.DMA((CHUNKS,))],
        compiler_params=params(),
        name="gain_grad",
    )(weight, in_hbm(products))


def attend_body(place, gain, weight, m0, m1, m2, m3, o0, o1, o2, o3, tokens, asked, arrivals):
    copies = []
    for r, message in enumerate((m0, m1, m2, m3)):
        x = pltpu.make_async_copy(message.at[pl.ds(0, TOK)], tokens.at[r], arrivals.at[r, 0])
        q = pltpu.make_async_copy(message.at[pl.ds(QROW, DEC)], asked.at[r], arrivals.at[r, 1])
        x.start()
        q.start()
        copies.append((x, q))
    rows = GH * DEC
    row_head = lax.broadcasted_iota(jnp.int32, (rows, COLS), 0) // DEC
    col_head = lax.broadcasted_iota(jnp.int32, (rows, COLS), 1) // HEAD_DIM
    same = row_head == col_head
    spot = (lax.broadcasted_iota(jnp.int32, (1, TOK), 1) // LEN).astype(jnp.float32)
    upper = place[1] == 1
    for r, out in enumerate((o0, o1, o2, o3)):
        for copy in copies[r]:
            copy.wait()
        values = tokens[r].astype(jnp.float32)
        scaled = (values * inverse_rms(values) * gain[...]).astype(jnp.bfloat16)
        states = jnp.dot(scaled, weight[...], preferred_element_type=jnp.float32).astype(jnp.bfloat16)
        query = jnp.where(
            upper,
            asked[r, :, COLS : 2 * COLS].astype(jnp.float32),
            asked[r, :, :COLS].astype(jnp.float32),
        )
        spread = jnp.where(same, jnp.concatenate([query] * GH, axis=0), 0.0).astype(jnp.bfloat16)
        scores = lax.dot_general(
            spread, states[:, :COLS], (((1,), (1,)), ((), ())), preferred_element_type=jnp.float32
        ) * HEAD_DIM ** (-0.5)
        count = asked[r, :, 2 * COLS : 2 * COLS + TOK].astype(jnp.float32)[0:1, :]
        scores = jnp.where(spot < count, scores, -jnp.inf)
        raised = jnp.exp(scores - jnp.max(scores, axis=-1, keepdims=True))
        weights = (raised / jnp.sum(raised, axis=-1, keepdims=True)).astype(jnp.bfloat16)
        mixed = jnp.dot(weights, states[:, COLS:], preferred_element_type=jnp.float32)
        mixed = jnp.where(same, mixed, 0.0).reshape(GH, DEC, COLS)
        out[...] = jnp.sum(mixed, axis=0).astype(jnp.bfloat16)


def attend(place, gain, weight, messages):
    return pl.pallas_call(
        attend_body,
        out_shape=tuple(jax.ShapeDtypeStruct((DEC, COLS), jnp.bfloat16) for _ in range(G)),
        in_specs=[SM, VM, VM] + [HB] * G,
        out_specs=(VM,) * G,
        scratch_shapes=[
            pltpu.VMEM((G, TOK, D), jnp.bfloat16),
            pltpu.VMEM((G, DEC, D), jnp.bfloat16),
            pltpu.SemaphoreType.DMA((G, 2)),
        ],
        compiler_params=params(),
        name="attend",
    )(place, gain, weight, *map(in_hbm, messages))


def assemble_body(member, p0, p1, p2, p3, out):
    parts = (p0, p1, p2, p3)
    for g in range(G):

        @pl.when(member[0] == g)
        def _():
            for j in range(G):
                out[:, j * COLS : (j + 1) * COLS] = parts[j ^ g][...]


def assemble(member, parts):
    return pl.pallas_call(
        assemble_body,
        out_shape=jax.ShapeDtypeStruct((DEC, HW), jnp.bfloat16),
        in_specs=[SM] + [VM] * G,
        out_specs=VM,
        compiler_params=params(),
        name="assemble",
    )(member, *parts)


def exchange(array, axes):
    return lax.all_to_all(array, axes, 0, 0, tiled=True)


def spread_to(array, axis):
    return exchange(jnp.broadcast_to(array[None], (lax.axis_size(axis), *array.shape)), axis)


def swap(array, axis):
    return lax.ppermute(array, axis, [(0, 1), (1, 0)])


def forward(passages, counts, helper_table, norm_gain, projection, queries, cotangent):
    zl, core = lax.axis_index("zl").astype(jnp.int32), lax.axis_index("core").astype(jnp.int32)
    place = jnp.stack([zl, core])
    member = (zl * 2 + core).reshape(1)
    gain = norm_gain.reshape(1, D)

    near, far = prep(
        place, counts.reshape(1), passages.reshape(TOK, D), cotangent.reshape(ENC * LEN, D), queries.reshape(DEC, HW)
    )
    m_z = swap(far, "zl")
    m_c = swap(near, "core")
    m_cz = swap(m_z, "core")
    messages = (near, m_c, m_z, m_cz)

    outgoing = pack(helper_table.reshape(2, PMAX - KEEP), passages.reshape(PMAX, LEN, D))
    arrived = exchange(outgoing, FSDP)
    mine = columns(member, projection)
    mine, arrived = lax.optimization_barrier((mine, arrived))
    by_y = exchange(mine, "y").reshape(512, 2 * COLS)

    tags = arrived[:, 0, D].astype(jnp.int32)
    h_own = unpack(tags, arrived).reshape(AID, D)
    h_z = swap(h_own, "zl")
    h_c = swap(h_own, "core")
    h_cz = swap(h_z, "core")
    weight = spread_to(by_y, "x").reshape(D, 2 * COLS)
    products = outer(place, messages, (h_own, h_c, h_z, h_cz))

    row_terms = grad(weight, products)
    parts = exchange(row_terms.reshape(32, 1, 64), FSDP)
    share = jnp.sum(parts, axis=0)
    gathered = exchange(jnp.broadcast_to(share[None], (16, 1, 64)), DP)
    gradient = jnp.sum(gathered, axis=0).reshape(64)

    mixed = attend(place, gain, weight, messages)
    from_core = swap(mixed[1], "core")
    from_z = swap(mixed[2], "zl")
    from_both = lax.ppermute(mixed[3], GROUP, [(i, i ^ 3) for i in range(G)])
    context_out = assemble(member, (mixed[0], from_core, from_z, from_both)).reshape(1, 1, DEC, HW)
    return (context_out, gradient)


def solution(mesh):
    split = Mesh(mesh.devices.reshape(4, 2, 2, 4, 8), ("zh", "zl", "core", "x", "y"))
    return jax.shard_map(
        forward,
        mesh=split,
        in_specs=(
            P(DP, FSDP, None, None, None),
            P(DP, FSDP),
            P(DP, FSDP, None, None),
            P(),
            P(FSDP, None),
            P(DP, FSDP, None, None),
            P(DP, FSDP, None, None, None),
        ),
        out_specs=(P(DP, FSDP, None, None), P(FSDP)),
        check_vma=False,
    )
```

```python
import jax
import jax.numpy as jnp
from jax import lax
from jax.experimental import pallas as pl
from jax.experimental.pallas import tpu as pltpu
from jax.sharding import Mesh
from jax.sharding import PartitionSpec as P

D = 2048
HEADS = 32
HEAD_DIM = 32
HW = 1024
DEC = 16
LEN = 8
PMAX = 40
KEEP = 8
HELP = 16
ENC = 24
TOK = PMAX * LEN
OWN = KEEP * LEN
AID = HELP * LEN
G = 4
COLS = HW // G
GH = HEADS // G
CROW = TOK + ENC * LEN // 2
QROW = CROW
MROWS = QROW + DEC
WIDE = D + 128
EPSILON = 1e-06
BLOCK = 512
GROUP = ("zl", "core")
DP = ("zh", "zl", "core")
FSDP = ("x", "y")

VM = pl.BlockSpec(memory_space=pltpu.VMEM)
SM = pl.BlockSpec(memory_space=pltpu.SMEM)
HB = pl.BlockSpec(memory_space=pltpu.HBM)


def in_hbm(array):
    return pltpu.with_memory_space_constraint(array, pltpu.HBM)


def params():
    return pltpu.CompilerParams(vmem_limit_bytes=24 * 1024 * 1024)


def pack_body(table, passages, out, arrivals):
    def copy(e):
        peer = jnp.maximum(table[0, e], 0)
        return pltpu.make_async_copy(passages.at[KEEP + e], out.at[peer, :, pl.ds(0, D)], arrivals.at[e])

    for e in range(PMAX - KEEP):

        @pl.when(table[0, e] >= 0)
        def _():
            copy(e).start()

    for s in range(32):
        out[s, :, D:] = jnp.full((LEN, WIDE - D), -1.0, jnp.bfloat16)
    for e in range(PMAX - KEEP):
        peer = table[0, e]

        @pl.when(peer >= 0)
        def _():
            slot = table[1, e].astype(jnp.float32)
            out[peer, :, D:] = jnp.full((LEN, WIDE - D), slot, jnp.float32).astype(jnp.bfloat16)

    for e in range(PMAX - KEEP):

        @pl.when(table[0, e] >= 0)
        def _():
            copy(e).wait()


def pack(table, passages):
    return pl.pallas_call(
        pack_body,
        out_shape=jax.ShapeDtypeStruct((32, LEN, WIDE), jnp.bfloat16),
        in_specs=[SM, HB],
        out_specs=VM,
        scratch_shapes=[pltpu.SemaphoreType.DMA((PMAX - KEEP,))],
        compiler_params=params(),
        name="pack",
    )(table, in_hbm(passages))


def prep_body(place, count, passages, cot, queries, near, far):
    half = ENC * LEN // 2
    for out, flip in ((near, 0), (far, 1)):
        out[:TOK, :] = passages[...]
        for z in range(2):

            @pl.when(place[0] == z)
            def _():
                for c in range(2):
                    lo = (2 * (z ^ flip) + c) * COLS
                    for part in range(2):
                        at = (2 * c + part) * 2 * COLS
                        rows = slice(part * half, (part + 1) * half)
                        out[TOK:CROW, at : at + COLS] = cot[rows, lo : lo + COLS]
                        out[TOK:CROW, at + COLS : at + 2 * COLS] = cot[rows, HW + lo : HW + lo + COLS]
                    out[QROW:, c * COLS : (c + 1) * COLS] = queries[:, lo : lo + COLS]

        out[QROW:, 2 * COLS :] = jnp.full((DEC, D - 2 * COLS), count[0].astype(jnp.float32), jnp.float32).astype(
            jnp.bfloat16
        )


def prep(place, count, passages, cot, queries):
    message = jax.ShapeDtypeStruct((MROWS, D), jnp.bfloat16)
    return pl.pallas_call(
        prep_body,
        out_shape=(message, message),
        in_specs=[SM, SM, VM, VM, VM],
        out_specs=(VM, VM),
        compiler_params=params(),
        name="prep",
    )(place, count, passages, cot, queries)


def columns_body(member, projection, out):
    for g in range(G):

        @pl.when(member[0] == g)
        def _():
            lo = g * COLS
            for peer in range(8):
                out[peer, :, :COLS] = projection[:, lo : lo + COLS]
                out[peer, :, COLS:] = projection[:, HW + lo : HW + lo + COLS]


def columns(member, projection):
    return pl.pallas_call(
        columns_body,
        out_shape=jax.ShapeDtypeStruct((8, 64, 2 * COLS), jnp.bfloat16),
        in_specs=[SM, VM],
        out_specs=VM,
        compiler_params=params(),
        name="columns",
    )(member, projection)


def unpack_body(tags, arrived, out):
    out[...] = jnp.zeros(out.shape, out.dtype)
    for s in range(32):
        tag = tags[s]

        @pl.when(tag >= 0)
        def _():
            out[tag] = arrived[s, :, :D]


def unpack(tags, arrived):
    return pl.pallas_call(
        unpack_body,
        out_shape=jax.ShapeDtypeStruct((HELP, LEN, D), jnp.bfloat16),
        in_specs=[SM, VM],
        out_specs=VM,
        compiler_params=params(),
        name="unpack",
    )(tags, arrived)


def inverse_rms(values):
    return lax.rsqrt(jnp.mean(values * values, axis=-1, keepdims=True) + EPSILON)


def block_rows(ring, step):
    return pl.ds(pl.multiple_of(((ring[0] + step) % 4) * BLOCK, BLOCK), BLOCK)


def weight_body(ring, own, left, right, top, bottom, out):
    half = BLOCK // 2
    out[block_rows(ring, 0), :] = own[...]
    out[block_rows(ring, 3), :] = left[...]
    out[block_rows(ring, 1), :] = right[...]
    far = pl.multiple_of(((ring[0] + 2) % 4) * BLOCK, BLOCK)
    out[pl.ds(far, half), :] = top[...]
    out[pl.ds(pl.multiple_of(far + half, half), half), :] = bottom[...]


def join_weight(ring, pieces):
    return pl.pallas_call(
        weight_body,
        out_shape=jax.ShapeDtypeStruct((D, 2 * COLS), jnp.bfloat16),
        in_specs=[SM] + [VM] * 5,
        out_specs=VM,
        compiler_params=params(),
        name="join_weight",
    )(ring, *pieces)


def grad_body(place, weight, m0, m1, h0, h1, *refs):
    *base, out, normal, tails, cots, own, row, arrivals = refs
    size = ENC * LEN
    copies = []
    for r, message in enumerate((m0, m1)):
        head = pltpu.make_async_copy(message.at[pl.ds(0, OWN)], own.at[r], arrivals.at[r, 0])
        tail = pltpu.make_async_copy(message.at[pl.ds(TOK, MROWS - TOK)], tails.at[r], arrivals.at[r, 1])
        head.start()
        tail.start()
        copies.append((head, tail))
    spot = (lax.broadcasted_iota(jnp.int32, (OWN, 1), 0) // LEN).astype(jnp.float32)
    for r, aid in enumerate((h0, h1)):
        at = r * size
        helped = aid[...].astype(jnp.float32)
        normal[at + OWN : at + size, :] = helped * inverse_rms(helped)
        for copy in copies[r]:
            copy.wait()
        count = tails[r, QROW - TOK :, 2 * COLS : 2 * COLS + 128].astype(jnp.float32)[0:1, 0:1]
        values = own[r].astype(jnp.float32)
        normal[at : at + OWN, :] = values * jnp.where(spot < count, inverse_rms(values), 0.0)
        for c in range(2):

            @pl.when(place[1] == c)
            def _():
                left = 4 * c * COLS
                half = size // 2
                cots[at : at + half, :] = tails[r, :half, left : left + 2 * COLS]
                cots[at + half : at + size, :] = tails[r, :half, left + 2 * COLS : left + 4 * COLS]

    for d in range(0, D, BLOCK):
        back = lax.dot_general(
            cots[...], weight[d : d + BLOCK, :], (((1,), (1,)), ((), ())), preferred_element_type=jnp.float32
        )
        row[:, d : d + BLOCK] = jnp.sum(normal[:, d : d + BLOCK] * back, axis=0, keepdims=True)
    for f in range(32):
        terms = row[:, f * 64 : (f + 1) * 64]
        if base:
            terms = terms + base[0][f : f + 1, :]
        out[f : f + 1, :] = terms


def grad(place, weight, messages, hs, base=None):
    extra = () if base is None else (base,)
    return pl.pallas_call(
        grad_body,
        out_shape=jax.ShapeDtypeStruct((32, 64), jnp.float32),
        in_specs=[SM, VM] + [HB] * 2 + [VM] * (2 + len(extra)),
        out_specs=VM,
        scratch_shapes=[
            pltpu.VMEM((2 * ENC * LEN, D), jnp.float32),
            pltpu.VMEM((2, MROWS - TOK, D), jnp.bfloat16),
            pltpu.VMEM((2 * ENC * LEN, 2 * COLS), jnp.bfloat16),
            pltpu.VMEM((2, OWN, D), jnp.bfloat16),
            pltpu.VMEM((1, D), jnp.float32),
            pltpu.SemaphoreType.DMA((2, 2)),
        ],
        compiler_params=params(),
        name="gain_grad",
    )(place, weight, *map(in_hbm, messages), *hs, *extra)


def attend_body(place, gain, weight, m0, m1, m2, m3, o0, o1, o2, o3, tokens, asked, arrivals):
    copies = []
    for r, message in enumerate((m0, m1, m2, m3)):
        x = pltpu.make_async_copy(message.at[pl.ds(0, TOK)], tokens.at[r], arrivals.at[r, 0])
        q = pltpu.make_async_copy(message.at[pl.ds(QROW, DEC)], asked.at[r], arrivals.at[r, 1])
        x.start()
        q.start()
        copies.append((x, q))
    rows = GH * DEC
    row_head = lax.broadcasted_iota(jnp.int32, (rows, COLS), 0) // DEC
    col_head = lax.broadcasted_iota(jnp.int32, (rows, COLS), 1) // HEAD_DIM
    same = row_head == col_head
    spot = (lax.broadcasted_iota(jnp.int32, (1, TOK), 1) // LEN).astype(jnp.float32)
    upper = place[1] == 1
    for r, out in enumerate((o0, o1, o2, o3)):
        for copy in copies[r]:
            copy.wait()
        values = tokens[r].astype(jnp.float32)
        scaled = (values * inverse_rms(values) * gain[...]).astype(jnp.bfloat16)
        states = jnp.dot(scaled, weight[...], preferred_element_type=jnp.float32).astype(jnp.bfloat16)
        query = jnp.where(
            upper,
            asked[r, :, COLS : 2 * COLS].astype(jnp.float32),
            asked[r, :, :COLS].astype(jnp.float32),
        )
        spread = jnp.where(same, jnp.concatenate([query] * GH, axis=0), 0.0).astype(jnp.bfloat16)
        scores = lax.dot_general(
            spread, states[:, :COLS], (((1,), (1,)), ((), ())), preferred_element_type=jnp.float32
        ) * HEAD_DIM ** (-0.5)
        count = asked[r, :, 2 * COLS : 2 * COLS + TOK].astype(jnp.float32)[0:1, :]
        scores = jnp.where(spot < count, scores, -jnp.inf)
        raised = jnp.exp(scores - jnp.max(scores, axis=-1, keepdims=True))
        weights = (raised / jnp.sum(raised, axis=-1, keepdims=True)).astype(jnp.bfloat16)
        mixed = jnp.dot(weights, states[:, COLS:], preferred_element_type=jnp.float32)
        mixed = jnp.where(same, mixed, 0.0).reshape(GH, DEC, COLS)
        out[...] = jnp.sum(mixed, axis=0).astype(jnp.bfloat16)


def attend(place, gain, weight, messages):
    return pl.pallas_call(
        attend_body,
        out_shape=tuple(jax.ShapeDtypeStruct((DEC, COLS), jnp.bfloat16) for _ in range(G)),
        in_specs=[SM, VM, VM] + [HB] * G,
        out_specs=(VM,) * G,
        scratch_shapes=[
            pltpu.VMEM((G, TOK, D), jnp.bfloat16),
            pltpu.VMEM((G, DEC, D), jnp.bfloat16),
            pltpu.SemaphoreType.DMA((G, 2)),
        ],
        compiler_params=params(),
        name="attend",
    )(place, gain, weight, *map(in_hbm, messages))


def assemble_body(member, p0, p1, p2, p3, out):
    parts = (p0, p1, p2, p3)
    for g in range(G):

        @pl.when(member[0] == g)
        def _():
            for j in range(G):
                out[:, j * COLS : (j + 1) * COLS] = parts[j ^ g][...]


def assemble(member, parts):
    return pl.pallas_call(
        assemble_body,
        out_shape=jax.ShapeDtypeStruct((DEC, HW), jnp.bfloat16),
        in_specs=[SM] + [VM] * G,
        out_specs=VM,
        compiler_params=params(),
        name="assemble",
    )(member, *parts)


def exchange(array, axes):
    return lax.all_to_all(array, axes, 0, 0, tiled=True)


def swap(array, axis):
    return lax.ppermute(array, axis, [(0, 1), (1, 0)])


def turn(array, step):
    return lax.ppermute(array, "x", [(i, (i + step) % 4) for i in range(4)])


def forward(passages, counts, helper_table, norm_gain, projection, queries, cotangent):
    zl, core = lax.axis_index("zl").astype(jnp.int32), lax.axis_index("core").astype(jnp.int32)
    place = jnp.stack([zl, core])
    member = (zl * 2 + core).reshape(1)
    gain = norm_gain.reshape(1, D)

    ring = lax.axis_index("x").astype(jnp.int32).reshape(1)

    mine = columns(member, projection)
    by_y = exchange(mine, "y").reshape(BLOCK, 2 * COLS)

    near, far = prep(
        place,
        counts.reshape(1),
        passages.reshape(TOK, D),
        cotangent.reshape(ENC * LEN, D),
        queries.reshape(DEC, HW),
    )
    m_z = swap(far, "zl")
    m_c = swap(near, "core")
    m_cz = swap(m_z, "core")
    messages = (near, m_c, m_z, m_cz)

    outgoing = pack(helper_table.reshape(2, PMAX - KEEP), passages.reshape(PMAX, LEN, D))
    arrived = exchange(outgoing, FSDP)

    left = turn(by_y, 1)
    right = turn(by_y, 3)
    top = turn(left[: BLOCK // 2], 1)
    bottom = turn(right[BLOCK // 2 :], 3)
    weight = join_weight(ring, (by_y, left, right, top, bottom))

    tags = arrived[:, 0, D].astype(jnp.int32)
    h_own = unpack(tags, arrived).reshape(AID, D)
    h_z = swap(h_own, "zl")
    h_c = swap(h_own, "core")
    h_cz = swap(h_z, "core")

    mixed = attend(place, gain, weight, messages)
    from_core = swap(mixed[1], "core")
    from_z = swap(mixed[2], "zl")
    from_both = lax.ppermute(mixed[3], GROUP, [(i, i ^ 3) for i in range(G)])
    context_out = assemble(member, (mixed[0], from_core, from_z, from_both)).reshape(1, 1, DEC, HW)

    row_terms = grad(place, weight, (near, m_c), (h_own, h_c))
    row_terms = grad(place, weight, (m_z, m_cz), (h_z, h_cz), row_terms)
    parts = exchange(row_terms.reshape(32, 1, 64), FSDP)
    share = jnp.sum(parts, axis=0)
    gathered = exchange(jnp.broadcast_to(share[None], (16, 1, 64)), DP)
    gradient = jnp.sum(gathered, axis=0).reshape(64)
    return (context_out, gradient)


def solution(mesh):
    split = Mesh(mesh.devices.reshape(4, 2, 2, 4, 8), ("zh", "zl", "core", "x", "y"))
    return jax.shard_map(
        forward,
        mesh=split,
        in_specs=(
            P(DP, FSDP, None, None, None),
            P(DP, FSDP),
            P(DP, FSDP, None, None),
            P(),
            P(FSDP, None),
            P(DP, FSDP, None, None),
            P(DP, FSDP, None, None, None),
        ),
        out_specs=(P(DP, FSDP, None, None), P(FSDP)),
        check_vma=False,
    )
```

```python
import functools

import jax
import jax.numpy as jnp
from jax import lax
from jax.experimental import pallas as pl
from jax.experimental.pallas import tpu as pltpu
from jax.sharding import Mesh
from jax.sharding import PartitionSpec as P

D = 2048
HEADS = 32
HEAD_DIM = 32
HW = 1024
DEC = 16
LEN = 8
PMAX = 40
KEEP = 8
HELP = 16
ENC = 24
TOK = PMAX * LEN
OWN = KEEP * LEN
AID = HELP * LEN
G = 4
COLS = HW // G
GH = HEADS // G
CROW = TOK + ENC * LEN // 2
QROW = CROW
MROWS = QROW + DEC
WIDE = D + 128
EPSILON = 1e-06
BLOCK = 512
GROUP = ("zl", "core")
DP = ("zh", "zl", "core")
FSDP = ("x", "y")

VM = pl.BlockSpec(memory_space=pltpu.VMEM)
SM = pl.BlockSpec(memory_space=pltpu.SMEM)
HB = pl.BlockSpec(memory_space=pltpu.HBM)


def in_hbm(array):
    return pltpu.with_memory_space_constraint(array, pltpu.HBM)


def params():
    return pltpu.CompilerParams(vmem_limit_bytes=24 * 1024 * 1024)


def pack_body(table, passages, out, arrivals):
    def copy(e):
        peer = jnp.maximum(table[0, e], 0)
        return pltpu.make_async_copy(passages.at[KEEP + e], out.at[peer, :, pl.ds(0, D)], arrivals.at[e])

    for e in range(PMAX - KEEP):

        @pl.when(table[0, e] >= 0)
        def _():
            copy(e).start()

    for s in range(32):
        out[s, :, D:] = jnp.full((LEN, WIDE - D), -1.0, jnp.bfloat16)
    for e in range(PMAX - KEEP):
        peer = table[0, e]

        @pl.when(peer >= 0)
        def _():
            slot = table[1, e].astype(jnp.float32)
            out[peer, :, D:] = jnp.full((LEN, WIDE - D), slot, jnp.float32).astype(jnp.bfloat16)

    for e in range(PMAX - KEEP):

        @pl.when(table[0, e] >= 0)
        def _():
            copy(e).wait()


def pack(table, passages):
    return pl.pallas_call(
        pack_body,
        out_shape=jax.ShapeDtypeStruct((32, LEN, WIDE), jnp.bfloat16),
        in_specs=[SM, HB],
        out_specs=VM,
        scratch_shapes=[pltpu.SemaphoreType.DMA((PMAX - KEEP,))],
        compiler_params=params(),
        name="pack",
    )(table, in_hbm(passages))


def prep_body(place, count, passages, cot, queries, near, far):
    half = ENC * LEN // 2
    for out, flip in ((near, 0), (far, 1)):
        out[:TOK, :] = passages[...]
        for z in range(2):

            @pl.when(place[0] == z)
            def _():
                for c in range(2):
                    lo = (2 * (z ^ flip) + c) * COLS
                    for part in range(2):
                        at = (2 * c + part) * 2 * COLS
                        rows = slice(part * half, (part + 1) * half)
                        out[TOK:CROW, at : at + COLS] = cot[rows, lo : lo + COLS]
                        out[TOK:CROW, at + COLS : at + 2 * COLS] = cot[rows, HW + lo : HW + lo + COLS]
                    out[QROW:, c * COLS : (c + 1) * COLS] = queries[:, lo : lo + COLS]

        out[QROW:, 2 * COLS :] = jnp.full((DEC, D - 2 * COLS), count[0].astype(jnp.float32), jnp.float32).astype(
            jnp.bfloat16
        )


def prep(place, count, passages, cot, queries):
    message = jax.ShapeDtypeStruct((MROWS, D), jnp.bfloat16)
    return pl.pallas_call(
        prep_body,
        out_shape=(message, message),
        in_specs=[SM, SM, VM, VM, VM],
        out_specs=(VM, VM),
        compiler_params=params(),
        name="prep",
    )(place, count, passages, cot, queries)


def columns_body(member, projection, out):
    for g in range(G):

        @pl.when(member[0] == g)
        def _():
            lo = g * COLS
            for peer in range(8):
                out[peer, :, :COLS] = projection[:, lo : lo + COLS]
                out[peer, :, COLS:] = projection[:, HW + lo : HW + lo + COLS]


def columns(member, projection):
    return pl.pallas_call(
        columns_body,
        out_shape=jax.ShapeDtypeStruct((8, 64, 2 * COLS), jnp.bfloat16),
        in_specs=[SM, VM],
        out_specs=VM,
        compiler_params=params(),
        name="columns",
    )(member, projection)


def unpack_body(tags, arrived, out):
    out[...] = jnp.zeros(out.shape, out.dtype)
    for s in range(32):
        tag = tags[s]

        @pl.when(tag >= 0)
        def _():
            out[tag] = arrived[s, :, :D]


def unpack(tags, arrived):
    return pl.pallas_call(
        unpack_body,
        out_shape=jax.ShapeDtypeStruct((HELP, LEN, D), jnp.bfloat16),
        in_specs=[SM, VM],
        out_specs=VM,
        compiler_params=params(),
        name="unpack",
    )(tags, arrived)


def inverse_rms(values):
    return lax.rsqrt(jnp.mean(values * values, axis=-1, keepdims=True) + EPSILON)


def block_rows(ring, step):
    return pl.ds(pl.multiple_of(((ring[0] + step) % 4) * BLOCK, BLOCK), BLOCK)


def weight_body(ring, own, left, right, far, out):
    for step, piece in ((0, own), (3, left), (1, right), (2, far)):
        out[block_rows(ring, step), :] = piece[...]


def join_weight(ring, pieces):
    return pl.pallas_call(
        weight_body,
        out_shape=jax.ShapeDtypeStruct((D, 2 * COLS), jnp.bfloat16),
        in_specs=[SM] + [VM] * 4,
        out_specs=VM,
        compiler_params=params(),
        name="join_weight",
    )(ring, *pieces)


def scale_body(message, gain, out):
    values = message[...].astype(jnp.float32)
    out[...] = (values * inverse_rms(values) * gain[...]).astype(jnp.bfloat16)


def scale(message, gain):
    return pl.pallas_call(
        scale_body,
        out_shape=pltpu.HBM((TOK, D), jnp.bfloat16),
        grid=(1,),
        in_specs=[pl.BlockSpec((TOK, D), lambda i: (0, 0)), pl.BlockSpec((1, D), lambda i: (0, 0))],
        out_specs=pl.BlockSpec((TOK, D), lambda i: (0, 0)),
        compiler_params=params(),
        name="scale",
    )(in_hbm(message), gain)


def grad_body(place, weight, m0, m1, m2, m3, h0, h1, h2, h3, out, normal, tails, cots, own, row, arrivals):
    size = ENC * LEN
    copies = []
    for r, message in enumerate((m0, m1, m2, m3)):
        head = pltpu.make_async_copy(message.at[pl.ds(0, OWN)], own.at[r], arrivals.at[r, 0])
        tail = pltpu.make_async_copy(message.at[pl.ds(TOK, MROWS - TOK)], tails.at[r], arrivals.at[r, 1])
        head.start()
        tail.start()
        copies.append((head, tail))
    spot = (lax.broadcasted_iota(jnp.int32, (OWN, 1), 0) // LEN).astype(jnp.float32)
    for r, aid in enumerate((h0, h1, h2, h3)):
        at = r * size
        helped = aid[...].astype(jnp.float32)
        normal[at + OWN : at + size, :] = helped * inverse_rms(helped)
        for copy in copies[r]:
            copy.wait()
        count = tails[r, QROW - TOK :, 2 * COLS : 2 * COLS + 128].astype(jnp.float32)[0:1, 0:1]
        values = own[r].astype(jnp.float32)
        normal[at : at + OWN, :] = values * jnp.where(spot < count, inverse_rms(values), 0.0)
        for c in range(2):

            @pl.when(place[1] == c)
            def _():
                left = 4 * c * COLS
                half = size // 2
                cots[at : at + half, :] = tails[r, :half, left : left + 2 * COLS]
                cots[at + half : at + size, :] = tails[r, :half, left + 2 * COLS : left + 4 * COLS]

    for d in range(0, D, BLOCK):
        back = lax.dot_general(
            cots[...], weight[d : d + BLOCK, :], (((1,), (1,)), ((), ())), preferred_element_type=jnp.float32
        )
        row[:, d : d + BLOCK] = jnp.sum(normal[:, d : d + BLOCK] * back, axis=0, keepdims=True)
    for f in range(32):
        out[f : f + 1, :] = row[:, f * 64 : (f + 1) * 64]


def grad(place, weight, messages, hs):
    return pl.pallas_call(
        grad_body,
        out_shape=jax.ShapeDtypeStruct((32, 64), jnp.float32),
        in_specs=[SM, VM] + [HB] * G + [VM] * G,
        out_specs=VM,
        scratch_shapes=[
            pltpu.VMEM((G * ENC * LEN, D), jnp.float32),
            pltpu.VMEM((G, MROWS - TOK, D), jnp.bfloat16),
            pltpu.VMEM((G * ENC * LEN, 2 * COLS), jnp.bfloat16),
            pltpu.VMEM((G, OWN, D), jnp.bfloat16),
            pltpu.VMEM((1, D), jnp.float32),
            pltpu.SemaphoreType.DMA((G, 2)),
        ],
        compiler_params=params(),
        name="gain_grad",
    )(place, weight, *map(in_hbm, messages), *hs)


def attend_body(scaled, place, gain, weight, x0, x1, m0, m1, o0, o1, tokens, asked, states, arrivals):
    copies = []
    for r, (source, message) in enumerate(((x0, m0), (x1, m1))):
        x = pltpu.make_async_copy(source.at[pl.ds(0, TOK)], tokens.at[r], arrivals.at[r, 0])
        q = pltpu.make_async_copy(message.at[pl.ds(QROW, DEC)], asked.at[r], arrivals.at[r, 1])
        x.start()
        q.start()
        copies.append((x, q))
    rows = GH * DEC
    row_head = lax.broadcasted_iota(jnp.int32, (rows, COLS), 0) // DEC
    col_head = lax.broadcasted_iota(jnp.int32, (rows, COLS), 1) // HEAD_DIM
    same = row_head == col_head
    spot = (lax.broadcasted_iota(jnp.int32, (1, TOK), 1) // LEN).astype(jnp.float32)
    upper = place[1] == 1
    for r in range(2):
        for copy in copies[r]:
            copy.wait()
        x = tokens[r]
        if not scaled:
            values = x.astype(jnp.float32)
            x = (values * inverse_rms(values) * gain[...]).astype(jnp.bfloat16)
        states[r] = jnp.dot(x, weight[...], preferred_element_type=jnp.float32).astype(jnp.bfloat16)
    scores = []
    for r in range(2):
        query = jnp.where(
            upper,
            asked[r, :, COLS : 2 * COLS].astype(jnp.float32),
            asked[r, :, :COLS].astype(jnp.float32),
        )
        spread = jnp.where(same, jnp.concatenate([query] * GH, axis=0), 0.0).astype(jnp.bfloat16)
        score = lax.dot_general(
            spread, states[r, :, :COLS], (((1,), (1,)), ((), ())), preferred_element_type=jnp.float32
        ) * HEAD_DIM ** (-0.5)
        count = asked[r, :, 2 * COLS : 2 * COLS + TOK].astype(jnp.float32)[0:1, :]
        scores.append(jnp.where(spot < count, score, -jnp.inf))
    scores = jnp.concatenate(scores, axis=0)
    raised = jnp.exp(scores - jnp.max(scores, axis=-1, keepdims=True))
    weights = (raised / jnp.sum(raised, axis=-1, keepdims=True)).astype(jnp.bfloat16)
    for r, out in enumerate((o0, o1)):
        mixed = jnp.dot(
            weights[r * rows : (r + 1) * rows, :], states[r, :, COLS:], preferred_element_type=jnp.float32
        )
        mixed = jnp.where(same, mixed, 0.0).reshape(GH, DEC, COLS)
        out[...] = jnp.sum(mixed, axis=0).astype(jnp.bfloat16)


def attend(place, gain, weight, sources, messages, scaled):
    return pl.pallas_call(
        functools.partial(attend_body, scaled),
        out_shape=tuple(jax.ShapeDtypeStruct((DEC, COLS), jnp.bfloat16) for _ in range(2)),
        in_specs=[SM, VM, VM] + [HB] * 4,
        out_specs=(VM,) * 2,
        scratch_shapes=[
            pltpu.VMEM((2, TOK, D), jnp.bfloat16),
            pltpu.VMEM((2, DEC, D), jnp.bfloat16),
            pltpu.VMEM((2, TOK, 2 * COLS), jnp.bfloat16),
            pltpu.SemaphoreType.DMA((2, 2)),
        ],
        compiler_params=params(),
        name="attend",
    )(place, gain, weight, *map(in_hbm, sources), *map(in_hbm, messages))


def assemble_body(member, p0, p1, p2, p3, out):
    parts = (p0, p1, p2, p3)
    for g in range(G):

        @pl.when(member[0] == g)
        def _():
            for j in range(G):
                out[:, j * COLS : (j + 1) * COLS] = parts[j ^ g][...]


def assemble(member, parts):
    return pl.pallas_call(
        assemble_body,
        out_shape=jax.ShapeDtypeStruct((DEC, HW), jnp.bfloat16),
        in_specs=[SM] + [VM] * G,
        out_specs=VM,
        compiler_params=params(),
        name="assemble",
    )(member, *parts)


def exchange(array, axes):
    return lax.all_to_all(array, axes, 0, 0, tiled=True)


def swap(array, axis):
    return lax.ppermute(array, axis, [(0, 1), (1, 0)])


def turn(array, step):
    return lax.ppermute(array, "x", [(i, (i + step) % 4) for i in range(4)])


def forward(passages, counts, helper_table, norm_gain, projection, queries, cotangent):
    zl, core = lax.axis_index("zl").astype(jnp.int32), lax.axis_index("core").astype(jnp.int32)
    place = jnp.stack([zl, core])
    member = (zl * 2 + core).reshape(1)
    gain = norm_gain.reshape(1, D)

    ring = lax.axis_index("x").astype(jnp.int32).reshape(1)

    mine = columns(member, projection)
    by_y = exchange(mine, "y").reshape(BLOCK, 2 * COLS)

    near, far = prep(
        place,
        counts.reshape(1),
        passages.reshape(TOK, D),
        cotangent.reshape(ENC * LEN, D),
        queries.reshape(DEC, HW),
    )
    m_z = swap(far, "zl")
    m_c = swap(near, "core")
    m_cz = swap(m_z, "core")
    messages = (near, m_c, m_z, m_cz)

    outgoing = pack(helper_table.reshape(2, PMAX - KEEP), passages.reshape(PMAX, LEN, D))
    arrived = exchange(outgoing, FSDP)

    left = turn(by_y, 1)
    right = turn(by_y, 3)
    opposite = turn(left, 1)
    weight = join_weight(ring, (by_y, left, right, opposite))
    s_0 = scale(near, gain)
    s_1 = scale(m_c, gain)

    tags = arrived[:, 0, D].astype(jnp.int32)
    h_own = unpack(tags, arrived).reshape(AID, D)
    h_z = swap(h_own, "zl")
    h_c = swap(h_own, "core")
    h_cz = swap(h_z, "core")

    mixed_own, mixed_core = attend(place, gain, weight, (s_0, s_1), (near, m_c), True)
    mixed_z, mixed_both = attend(place, gain, weight, (m_z, m_cz), (m_z, m_cz), False)
    from_core = swap(mixed_core, "core")
    from_z = swap(mixed_z, "zl")
    from_both = lax.ppermute(mixed_both, GROUP, [(i, i ^ 3) for i in range(G)])
    context_out = assemble(member, (mixed_own, from_core, from_z, from_both)).reshape(1, 1, DEC, HW)

    row_terms = grad(place, weight, messages, (h_own, h_c, h_z, h_cz))
    parts = exchange(row_terms.reshape(32, 1, 64), FSDP)
    share = jnp.sum(parts, axis=0)
    gathered = exchange(jnp.broadcast_to(share[None], (16, 1, 64)), DP)
    gradient = jnp.sum(gathered, axis=0).reshape(64)
    return (context_out, gradient)


def solution(mesh):
    split = Mesh(mesh.devices.reshape(4, 2, 2, 4, 8), ("zh", "zl", "core", "x", "y"))
    return jax.shard_map(
        forward,
        mesh=split,
        in_specs=(
            P(DP, FSDP, None, None, None),
            P(DP, FSDP),
            P(DP, FSDP, None, None),
            P(),
            P(FSDP, None),
            P(DP, FSDP, None, None),
            P(DP, FSDP, None, None, None),
        ),
        out_specs=(P(DP, FSDP, None, None), P(FSDP)),
        check_vma=False,
    )
```

```python
import functools

import jax
import jax.numpy as jnp
from jax import lax
from jax.experimental import pallas as pl
from jax.experimental.pallas import tpu as pltpu
from jax.sharding import Mesh
from jax.sharding import PartitionSpec as P

D = 2048
HEADS = 32
HEAD_DIM = 32
HW = 1024
DEC = 16
LEN = 8
PMAX = 40
KEEP = 8
HELP = 16
ENC = 24
TOK = PMAX * LEN
OWN = KEEP * LEN
AID = HELP * LEN
G = 4
COLS = HW // G
GH = HEADS // G
CROW = TOK + ENC * LEN // 2
QROW = CROW
MROWS = QROW + DEC
WIDE = D + 128
EPSILON = 1e-06
BLOCK = 512
GROUP = ("zl", "core")
DP = ("zh", "zl", "core")
FSDP = ("x", "y")

VM = pl.BlockSpec(memory_space=pltpu.VMEM)
SM = pl.BlockSpec(memory_space=pltpu.SMEM)
HB = pl.BlockSpec(memory_space=pltpu.HBM)


def in_hbm(array):
    return pltpu.with_memory_space_constraint(array, pltpu.HBM)


def params():
    return pltpu.CompilerParams(vmem_limit_bytes=24 * 1024 * 1024)


def pack_body(table, passages, out, arrivals):
    def copy(e):
        peer = jnp.maximum(table[0, e], 0)
        return pltpu.make_async_copy(passages.at[KEEP + e], out.at[peer, :, pl.ds(0, D)], arrivals.at[e])

    for e in range(PMAX - KEEP):

        @pl.when(table[0, e] >= 0)
        def _():
            copy(e).start()

    for s in range(32):
        out[s, :, D:] = jnp.full((LEN, WIDE - D), -1.0, jnp.bfloat16)
    for e in range(PMAX - KEEP):
        peer = table[0, e]

        @pl.when(peer >= 0)
        def _():
            slot = table[1, e].astype(jnp.float32)
            out[peer, :, D:] = jnp.full((LEN, WIDE - D), slot, jnp.float32).astype(jnp.bfloat16)

    for e in range(PMAX - KEEP):

        @pl.when(table[0, e] >= 0)
        def _():
            copy(e).wait()


def pack(table, passages):
    return pl.pallas_call(
        pack_body,
        out_shape=jax.ShapeDtypeStruct((32, LEN, WIDE), jnp.bfloat16),
        in_specs=[SM, HB],
        out_specs=VM,
        scratch_shapes=[pltpu.SemaphoreType.DMA((PMAX - KEEP,))],
        compiler_params=params(),
        name="pack",
    )(table, in_hbm(passages))


def prep_body(place, count, passages, cot, queries, near, far):
    half = ENC * LEN // 2
    for out, flip in ((near, 0), (far, 1)):
        out[:TOK, :] = passages[...]
        for z in range(2):

            @pl.when(place[0] == z)
            def _():
                for c in range(2):
                    lo = (2 * (z ^ flip) + c) * COLS
                    for part in range(2):
                        at = (2 * c + part) * 2 * COLS
                        rows = slice(part * half, (part + 1) * half)
                        out[TOK:CROW, at : at + COLS] = cot[rows, lo : lo + COLS]
                        out[TOK:CROW, at + COLS : at + 2 * COLS] = cot[rows, HW + lo : HW + lo + COLS]
                    out[QROW:, c * COLS : (c + 1) * COLS] = queries[:, lo : lo + COLS]

        out[QROW:, 2 * COLS :] = jnp.full((DEC, D - 2 * COLS), count[0].astype(jnp.float32), jnp.float32).astype(
            jnp.bfloat16
        )


def prep(place, count, passages, cot, queries):
    message = jax.ShapeDtypeStruct((MROWS, D), jnp.bfloat16)
    return pl.pallas_call(
        prep_body,
        out_shape=(message, message),
        in_specs=[SM, SM, VM, VM, VM],
        out_specs=(VM, VM),
        compiler_params=params(),
        name="prep",
    )(place, count, passages, cot, queries)


def columns_body(member, projection, out):
    for g in range(G):

        @pl.when(member[0] == g)
        def _():
            lo = g * COLS
            for peer in range(8):
                out[peer, :, :COLS] = projection[:, lo : lo + COLS]
                out[peer, :, COLS:] = projection[:, HW + lo : HW + lo + COLS]


def columns(member, projection):
    return pl.pallas_call(
        columns_body,
        out_shape=jax.ShapeDtypeStruct((8, 64, 2 * COLS), jnp.bfloat16),
        in_specs=[SM, VM],
        out_specs=VM,
        compiler_params=params(),
        name="columns",
    )(member, projection)


def unpack_body(tags, arrived, out):
    out[...] = jnp.zeros(out.shape, out.dtype)
    for s in range(32):
        tag = tags[s]

        @pl.when(tag >= 0)
        def _():
            out[tag] = arrived[s, :, :D]


def unpack(tags, arrived):
    return pl.pallas_call(
        unpack_body,
        out_shape=jax.ShapeDtypeStruct((HELP, LEN, D), jnp.bfloat16),
        in_specs=[SM, VM],
        out_specs=VM,
        compiler_params=params(),
        name="unpack",
    )(tags, arrived)


def inverse_rms(values):
    return lax.rsqrt(jnp.mean(values * values, axis=-1, keepdims=True) + EPSILON)


def block_rows(ring, step):
    return pl.ds(pl.multiple_of(((ring[0] + step) % 4) * BLOCK, BLOCK), BLOCK)


def weight_body(ring, own, left, right, far, out):
    for step, piece in ((0, own), (3, left), (1, right), (2, far)):
        out[block_rows(ring, step), :] = piece[...]


def join_weight(ring, pieces):
    return pl.pallas_call(
        weight_body,
        out_shape=jax.ShapeDtypeStruct((D, 2 * COLS), jnp.bfloat16),
        in_specs=[SM] + [VM] * 4,
        out_specs=VM,
        compiler_params=params(),
        name="join_weight",
    )(ring, *pieces)


def scale_body(message, gain, out):
    values = message[...].astype(jnp.float32)
    out[...] = (values * inverse_rms(values) * gain[...]).astype(jnp.bfloat16)


def scale(message, gain):
    return pl.pallas_call(
        scale_body,
        out_shape=pltpu.HBM((TOK, D), jnp.bfloat16),
        grid=(1,),
        in_specs=[pl.BlockSpec((TOK, D), lambda i: (0, 0)), pl.BlockSpec((1, D), lambda i: (0, 0))],
        out_specs=pl.BlockSpec((TOK, D), lambda i: (0, 0)),
        compiler_params=params(),
        name="scale",
    )(in_hbm(message), gain)


def grad_body(place, weight, m0, m1, m2, m3, h0, h1, h2, h3, out, normal, tails, cots, own, row, arrivals):
    size = ENC * LEN
    copies = []
    for r, message in enumerate((m0, m1, m2, m3)):
        head = pltpu.make_async_copy(message.at[pl.ds(0, OWN)], own.at[r], arrivals.at[r, 0])
        tail = pltpu.make_async_copy(message.at[pl.ds(TOK, MROWS - TOK)], tails.at[r], arrivals.at[r, 1])
        head.start()
        tail.start()
        copies.append((head, tail))
    spot = (lax.broadcasted_iota(jnp.int32, (OWN, 1), 0) // LEN).astype(jnp.float32)
    for r, aid in enumerate((h0, h1, h2, h3)):
        at = r * size
        helped = aid[...].astype(jnp.float32)
        normal[at + OWN : at + size, :] = helped * inverse_rms(helped)
        for copy in copies[r]:
            copy.wait()
        count = tails[r, QROW - TOK :, 2 * COLS : 2 * COLS + 128].astype(jnp.float32)[0:1, 0:1]
        values = own[r].astype(jnp.float32)
        normal[at : at + OWN, :] = values * jnp.where(spot < count, inverse_rms(values), 0.0)
        for c in range(2):

            @pl.when(place[1] == c)
            def _():
                left = 4 * c * COLS
                half = size // 2
                cots[at : at + half, :] = tails[r, :half, left : left + 2 * COLS]
                cots[at + half : at + size, :] = tails[r, :half, left + 2 * COLS : left + 4 * COLS]

    for d in range(0, D, BLOCK):
        back = lax.dot_general(
            cots[...], weight[d : d + BLOCK, :], (((1,), (1,)), ((), ())), preferred_element_type=jnp.float32
        )
        row[:, d : d + BLOCK] = jnp.sum(normal[:, d : d + BLOCK] * back, axis=0, keepdims=True)
    for f in range(32):
        out[f : f + 1, :] = row[:, f * 64 : (f + 1) * 64]


def grad(place, weight, messages, hs):
    return pl.pallas_call(
        grad_body,
        out_shape=jax.ShapeDtypeStruct((32, 64), jnp.float32),
        in_specs=[SM, VM] + [HB] * G + [VM] * G,
        out_specs=VM,
        scratch_shapes=[
            pltpu.VMEM((G * ENC * LEN, D), jnp.float32),
            pltpu.VMEM((G, MROWS - TOK, D), jnp.bfloat16),
            pltpu.VMEM((G * ENC * LEN, 2 * COLS), jnp.bfloat16),
            pltpu.VMEM((G, OWN, D), jnp.bfloat16),
            pltpu.VMEM((1, D), jnp.float32),
            pltpu.SemaphoreType.DMA((G, 2)),
        ],
        compiler_params=params(),
        name="gain_grad",
    )(place, weight, *map(in_hbm, messages), *hs)


def attend_body(scaled, place, gain, weight, x0, x1, m0, m1, o0, o1, tokens, asked, states, arrivals):
    copies = []
    for r, (source, message) in enumerate(((x0, m0), (x1, m1))):
        x = pltpu.make_async_copy(source.at[pl.ds(0, TOK)], tokens.at[r], arrivals.at[r, 0])
        q = pltpu.make_async_copy(message.at[pl.ds(QROW, DEC)], asked.at[r], arrivals.at[r, 1])
        x.start()
        q.start()
        copies.append((x, q))
    rows = GH * DEC
    row_head = lax.broadcasted_iota(jnp.int32, (rows, COLS), 0) // DEC
    col_head = lax.broadcasted_iota(jnp.int32, (rows, COLS), 1) // HEAD_DIM
    same = row_head == col_head
    spot = (lax.broadcasted_iota(jnp.int32, (1, TOK), 1) // LEN).astype(jnp.float32)
    upper = place[1] == 1
    for r in range(2):
        for copy in copies[r]:
            copy.wait()
        x = tokens[r]
        if not scaled:
            values = x.astype(jnp.float32)
            x = (values * inverse_rms(values) * gain[...]).astype(jnp.bfloat16)
        states[r] = jnp.dot(x, weight[...], preferred_element_type=jnp.float32).astype(jnp.bfloat16)
    scores = []
    for r in range(2):
        query = jnp.where(
            upper,
            asked[r, :, COLS : 2 * COLS].astype(jnp.float32),
            asked[r, :, :COLS].astype(jnp.float32),
        )
        spread = jnp.where(same, jnp.concatenate([query] * GH, axis=0), 0.0).astype(jnp.bfloat16)
        score = lax.dot_general(
            spread, states[r, :, :COLS], (((1,), (1,)), ((), ())), preferred_element_type=jnp.float32
        ) * HEAD_DIM ** (-0.5)
        count = asked[r, :, 2 * COLS : 2 * COLS + TOK].astype(jnp.float32)[0:1, :]
        scores.append(jnp.where(spot < count, score, -jnp.inf))
    scores = jnp.concatenate(scores, axis=0)
    raised = jnp.exp(scores - jnp.max(scores, axis=-1, keepdims=True))
    weights = (raised / jnp.sum(raised, axis=-1, keepdims=True)).astype(jnp.bfloat16)
    for r, out in enumerate((o0, o1)):
        mixed = jnp.dot(
            weights[r * rows : (r + 1) * rows, :], states[r, :, COLS:], preferred_element_type=jnp.float32
        )
        mixed = jnp.where(same, mixed, 0.0).reshape(GH, DEC, COLS)
        out[...] = jnp.sum(mixed, axis=0).astype(jnp.bfloat16)


def attend(place, gain, weight, sources, messages, scaled):
    return pl.pallas_call(
        functools.partial(attend_body, scaled),
        out_shape=tuple(jax.ShapeDtypeStruct((DEC, COLS), jnp.bfloat16) for _ in range(2)),
        in_specs=[SM, VM, VM] + [HB] * 4,
        out_specs=(VM,) * 2,
        scratch_shapes=[
            pltpu.VMEM((2, TOK, D), jnp.bfloat16),
            pltpu.VMEM((2, DEC, D), jnp.bfloat16),
            pltpu.VMEM((2, TOK, 2 * COLS), jnp.bfloat16),
            pltpu.SemaphoreType.DMA((2, 2)),
        ],
        compiler_params=params(),
        name="attend",
    )(place, gain, weight, *map(in_hbm, sources), *map(in_hbm, messages))


def assemble_body(member, p0, p1, p2, p3, out):
    parts = (p0, p1, p2, p3)
    for g in range(G):

        @pl.when(member[0] == g)
        def _():
            for j in range(G):
                out[:, j * COLS : (j + 1) * COLS] = parts[j ^ g][...]


def assemble(member, parts):
    return pl.pallas_call(
        assemble_body,
        out_shape=jax.ShapeDtypeStruct((DEC, HW), jnp.bfloat16),
        in_specs=[SM] + [VM] * G,
        out_specs=VM,
        compiler_params=params(),
        name="assemble",
    )(member, *parts)


def exchange(array, axes):
    return lax.all_to_all(array, axes, 0, 0, tiled=True)


def swap(array, axis):
    return lax.ppermute(array, axis, [(0, 1), (1, 0)])


def turn(array, step):
    return lax.ppermute(array, "x", [(i, (i + step) % 4) for i in range(4)])


def forward(passages, counts, helper_table, norm_gain, projection, queries, cotangent):
    zl, core = lax.axis_index("zl").astype(jnp.int32), lax.axis_index("core").astype(jnp.int32)
    place = jnp.stack([zl, core])
    member = (zl * 2 + core).reshape(1)
    gain = norm_gain.reshape(1, D)

    ring = lax.axis_index("x").astype(jnp.int32).reshape(1)

    mine = columns(member, projection)
    by_y = exchange(mine, "y").reshape(BLOCK, 2 * COLS)

    near, far = prep(
        place,
        counts.reshape(1),
        passages.reshape(TOK, D),
        cotangent.reshape(ENC * LEN, D),
        queries.reshape(DEC, HW),
    )
    m_z = swap(far, "zl")
    m_c = swap(near, "core")
    m_cz = swap(m_z, "core")
    messages = (near, m_c, m_z, m_cz)

    outgoing = pack(helper_table.reshape(2, PMAX - KEEP), passages.reshape(PMAX, LEN, D))
    arrived = exchange(outgoing, FSDP)

    left = turn(by_y, 1)
    right = turn(by_y, 3)
    onward = jnp.where(core == 0, left, right)
    opposite = lax.ppermute(
        onward, ("core", "x"), [(c * 4 + i, c * 4 + (i + (1, 3)[c]) % 4) for c in range(2) for i in range(4)]
    )
    weight = join_weight(ring, (by_y, left, right, opposite))
    s_0 = scale(near, gain)
    s_1 = scale(m_c, gain)

    tags = arrived[:, 0, D].astype(jnp.int32)
    h_own = unpack(tags, arrived).reshape(AID, D)
    h_z = swap(h_own, "zl")
    h_c = swap(h_own, "core")
    h_cz = swap(h_z, "core")

    mixed_own, mixed_core = attend(place, gain, weight, (s_0, s_1), (near, m_c), True)
    mixed_z, mixed_both = attend(place, gain, weight, (m_z, m_cz), (m_z, m_cz), False)
    from_core = swap(mixed_core, "core")
    from_z = swap(mixed_z, "zl")
    from_both = lax.ppermute(mixed_both, GROUP, [(i, i ^ 3) for i in range(G)])
    context_out = assemble(member, (mixed_own, from_core, from_z, from_both)).reshape(1, 1, DEC, HW)

    row_terms = grad(place, weight, messages, (h_own, h_c, h_z, h_cz))
    parts = exchange(row_terms.reshape(32, 1, 64), FSDP)
    share = jnp.sum(parts, axis=0)
    gathered = exchange(jnp.broadcast_to(share[None], (16, 1, 64)), DP)
    gradient = jnp.sum(gathered, axis=0).reshape(64)
    return (context_out, gradient)


def solution(mesh):
    split = Mesh(mesh.devices.reshape(4, 2, 2, 4, 8), ("zh", "zl", "core", "x", "y"))
    return jax.shard_map(
        forward,
        mesh=split,
        in_specs=(
            P(DP, FSDP, None, None, None),
            P(DP, FSDP),
            P(DP, FSDP, None, None),
            P(),
            P(FSDP, None),
            P(DP, FSDP, None, None),
            P(DP, FSDP, None, None, None),
        ),
        out_specs=(P(DP, FSDP, None, None), P(FSDP)),
        check_vma=False,
    )
```
